32 devices in a mesh: member: 2 (over y), pts: 4 (over x, core), sub: 4 (over z).
Axes of the slice: x: 2, y: 2, z: 4, core: 2. Of those that a mesh axis runs over, the one named last changes fastest.
Arguments:
- spectrum: bfloat16 [1800, 32, 512], P(None, ('member', 'pts'), 'sub'), parts along dimension 1, may hold values from 0.049804688 to 2
- interaction: bfloat16 [1800, 1800], replicated, may hold values from -0.125 to 0.125
- speeds: float32 [1800], replicated, may hold values from 0.2 to 0.7
- mask: int32 [16, 512], P('pts', 'sub'), may hold values from 0 to 1, as said below
Outputs:
- evolved: bfloat16 [1800, 32, 512], P(None, ('member', 'pts'), 'sub'), parts along dimension 1
The draws below stay inside these ranges and needn't reach their ends.
There are 2 independent parts, one for each index of `member`. The reference program is written for one: setup_inputs(seed, part) draws one part's arguments, and reference() takes and returns one part's arrays. A program takes and returns all parts, laid end to end along the dimension named above; an argument that names none is the same for every part. Nothing has to cross between parts.
Inputs may be any that keep to these rules, and one draw needn't show every extreme that they name: `mask`: 1 marks sea, 0 land; the share of sea differs from grid row to grid row.
All inputs are finite; a program needn't handle non-finite values.
Results may differ from the reference program's by a relative error of at most 0.0075.
Values may be sent and summed in bfloat16 or wider, within the bound.
A program may use at most 128 MiB of HBM per device.

```python
import math
import jax
import jax.numpy as jnp

ND = 36
PROP = 2
K = 1800
GX = 16
GY = 512


def draw_mask(key, part):
    row_key, cell_key = jax.random.split(jax.random.fold_in(key, 17))
    level = jax.random.randint(row_key, (GX, 1), 30, 96)
    roll = jax.random.randint(cell_key, (GX, GY), 0, 100)
    return (roll < level).astype(jnp.int32)


def block_scale(stream_key, shape, shards, least, top_value):
    def one(axis_at, shards_of):
        heights = jax.random.uniform(jax.random.fold_in(jax.random.fold_in(stream_key, 6), axis_at), (shards_of,), jnp.float32, least / len(shards), top_value / len(shards))
        return jnp.repeat(jnp.exp(heights), shape[axis_at] // shards_of).reshape((-1,) + (1,) * (len(shape) - axis_at - 1))

    loudness = one(*shards[0])
    for cut in shards[1:]:
        loudness = loudness * one(*cut)
    return loudness


def normal_values(key, dims, scale, reach, kind=jnp.bfloat16):
    array = jax.random.normal(key, dims, jnp.float32) * scale
    return jnp.minimum(jnp.maximum(array, -reach), reach).astype(kind)


def setup_inputs(seed: int = 0, part: int = 0) -> dict:
    keys = jax.random.split(jax.random.key(seed), 5)
    own_keys = jax.random.split(jax.random.fold_in(keys[4], part), 5)
    spectrum = jnp.clip(0.049804688 + 1.9501953 * jax.random.uniform(own_keys[0], (K, GX, GY), jnp.float32) ** block_scale(own_keys[0], (K, GX, GY), ((1, 4), (2, 4)), -0.2, 0.2), 0.049804688, 2.0).astype(jnp.bfloat16)
    interaction = normal_values(keys[1], (K, K), K ** -0.5, 0.125)
    speeds = jnp.clip(jnp.exp(jax.random.uniform(keys[2], (K,), jnp.float32, math.log(0.2), math.log(0.7))), 0.2, 0.7)
    mask = draw_mask(jax.random.fold_in(keys[4], 71), part)
    return {"spectrum": spectrum, "interaction": interaction, "speeds": speeds, "mask": mask}


coupling = 0.5


def advance(field, cross, along, sea):
    cross_up = jnp.maximum(cross, 0.0)
    cross_down = jnp.minimum(cross, 0.0)
    along_up = jnp.maximum(along, 0.0)
    along_down = jnp.minimum(along, 0.0)
    for substep in range(PROP):
        ext = jnp.pad(field, ((0, 0), (1, 1), (1, 1)))
        back_x = ext[:, :-2, 1:-1]
        next_x = ext[:, 2:, 1:-1]
        back_y = ext[:, 1:-1, :-2]
        next_y = ext[:, 1:-1, 2:]
        field = (field - cross_up * (field - back_x) - cross_down * (next_x - field)
                 - along_up * (field - back_y) - along_down * (next_y - field)) * sea
    return field


def reference(spectrum, interaction, speeds, mask):
    flat = spectrum.reshape(K, GX * GY)
    coupled = jnp.dot(interaction, flat, preferred_element_type=jnp.float32)
    wide = flat.astype(jnp.float32)
    sea_flat = mask.astype(jnp.float32).reshape(1, GX * GY)
    grown = ((wide + coupling * wide * coupled) * sea_flat).astype(jnp.bfloat16).reshape(K, GX, GY)
    index = jnp.arange(K, dtype=jnp.int32)
    angle = (index % ND).astype(jnp.float32) * jnp.float32(2.0 * math.pi / ND)
    cross = (speeds * jnp.cos(angle)).reshape(K, 1, 1)
    along = (speeds * jnp.sin(angle)).reshape(K, 1, 1)
    field = advance(grown.astype(jnp.float32), cross, along, mask.astype(jnp.float32)[None])
    return field.astype(jnp.bfloat16)
```

```python
import functools
import math

import jax
import jax.numpy as jnp
import numpy as np
from jax import lax
from jax.experimental import pallas as pl
from jax.experimental.pallas import tpu as pltpu
from jax.sharding import PartitionSpec as P

ND = 36
PROP = 2
UNIT = 72
SUB = 8
CHUNKS = 4

coupling = 0.5


def circle():
    angle = np.arange(ND, dtype=np.int32).astype(np.float32) * np.float32(2.0 * math.pi / ND)
    angle = angle.astype(np.float64)
    return np.cos(angle).astype(np.float32), np.sin(angle).astype(np.float32)


def runs(flags):
    found, start = [], None
    for i, flag in enumerate(list(flags) + [False]):
        if flag and start is None:
            start = i
        if not flag and start is not None:
            found.append((start, i - start))
            start = None
    return found


def tables(lanes):
    cosine, sine = circle()
    d = np.arange(UNIT) % ND
    rows = [np.abs(cosine[d]), np.abs(sine[d]), cosine[d] > 0, sine[d] > 0]
    return np.stack([np.broadcast_to(r.astype(np.float32)[:, None], (UNIT, lanes)) for r in rows])


def splits(blocks):
    size = max(2, blocks // CHUNKS // 2 * 2)
    starts = list(range(0, blocks, size))
    if len(starts) > 1 and blocks - starts[-1] < size:
        starts.pop()
    return [(s, (starts[i + 1] if i + 1 < len(starts) else blocks) - s) for i, s in enumerate(starts)]


def kernel(
    rows_x, chunks, plus_runs, minus_runs, counts,
    spec_hbm, inter_hbm, speeds_ref, mask_ref, tabs_ref, out_hbm,
    specv, inter, flat, acc, field, first, column, stage, packed, halo, outv,
    xsend, xrecv, ysend, yrecv,
    load_sem, out_sem, send_sem, recv_sem,
):
    lanes = flat.shape[1] // rows_x
    blocks = field.shape[1]
    tile_count = UNIT // SUB
    px, sy = lax.axis_index("pts"), lax.axis_index("sub")
    nx, ny = counts
    partner = [{"pts": px + 1}, {"pts": px - 1}, {"sub": sy + 1}, {"sub": sy - 1}]
    sends = [px < nx - 1, px > 0, sy < ny - 1, sy > 0]
    receives = [sends[1], sends[0], sends[3], sends[2]]

    spec_copy = pltpu.make_async_copy(spec_hbm, specv, load_sem.at[len(chunks)])
    spec_copy.start()
    inter_copies = []
    for c, (start, count) in enumerate(chunks):
        part = pl.ds(start * UNIT, count * UNIT)
        copy = pltpu.make_async_copy(inter_hbm.at[part], inter.at[part], load_sem.at[c])
        copy.start()
        inter_copies.append(copy)

    barrier = pltpu.get_barrier_semaphore()
    for kind in range(4):
        @pl.when(sends[kind])
        def _():
            pl.semaphore_signal(
                barrier, inc=1, device_id=partner[kind], device_id_type=pl.DeviceIdType.MESH
            )

    def exchange(e, c, kind):
        start, count = chunks[c]
        part = pl.ds(start, count)
        if kind < 2:
            source, target = xsend.at[e, kind, part], xrecv.at[e, kind, part]
        else:
            source, target = ysend.at[e, part], yrecv.at[e, kind - 2, part]
        return pltpu.make_async_remote_copy(
            src_ref=source, dst_ref=target,
            send_sem=send_sem.at[e, c, kind], recv_sem=recv_sem.at[e, c, kind],
            device_id=partner[kind], device_id_type=pl.DeviceIdType.MESH,
        )

    def start_sends(e, c):
        for kind in range(4):
            @pl.when(sends[kind])
            def _():
                exchange(e, c, kind).start()

    def wait_receives(e, c):
        for kind in range(4):
            @pl.when(receives[kind])
            def _():
                exchange(e, c, kind).wait_recv()

    for kind in range(4):
        @pl.when(jnp.logical_not(receives[kind]))
        def _():
            for e in range(PROP):
                if kind < 2:
                    xrecv[e, kind] = jnp.zeros(xrecv.shape[2:], xrecv.dtype)
                else:
                    yrecv[e, kind - 2] = jnp.zeros(yrecv.shape[2:], yrecv.dtype)

    for i in range(speeds_ref.shape[0]):
        row = jnp.broadcast_to(speeds_ref[i : i + 1, :], (lanes, lanes))
        column[i * lanes : (i + 1) * lanes, :] = row.T

    spec_copy.wait()

    def spread(block, count):
        length = count * UNIT
        whole = specv[pl.ds(pl.multiple_of(block * (rows_x * UNIT), 16), rows_x * length), :]
        stage[0 : rows_x * length, :] = whole.astype(jnp.float32)
        for x in range(rows_x):
            values = stage[pl.ds(x, length, stride=rows_x), :]
            flat[pl.ds(pl.multiple_of(block * UNIT, 16), length), x * lanes : (x + 1) * lanes] = (
                values.astype(jnp.bfloat16)
            )
            for b in range(count):
                field[x, block + b] = values[b * UNIT : (b + 1) * UNIT]

    @pl.loop(0, blocks // 2)
    def _(i):
        spread(2 * i, 2)

    if blocks % 2:
        spread(blocks - 1, 1)

    pl.semaphore_wait(barrier, sum(s.astype(jnp.int32) for s in sends))

    lane = lax.broadcasted_iota(jnp.int32, (SUB, lanes), 1)
    sea = [
        jnp.broadcast_to(mask_ref[x : x + 1, :].astype(jnp.float32), (UNIT, lanes))
        for x in range(rows_x)
    ]

    def pack(e, block, values):
        for kind, group, x in ((0, plus_runs, rows_x - 1), (1, minus_runs, 0)):
            at = 0
            for start, length in group:
                packed[kind, at : at + length, :] = values[x][start : start + length]
                at += length
            xsend[e, kind, block] = packed[kind].astype(xsend.dtype)
        message = jnp.zeros((SUB, lanes), jnp.float32)
        for t in range(tile_count):
            for x in range(rows_x):
                j = t * rows_x + x
                turned = pltpu.roll(values[x][t * SUB : (t + 1) * SUB], 2 * j + 1, 1)
                message = jnp.where((lane >= 2 * j) & (lane < 2 * j + 2), turned, message)
        ysend[e, block] = message

    def grow(c):
        start, count = chunks[c]

        @pl.loop(0, count)
        def _(i):
            block = start + i
            values = []
            for x in range(rows_x):
                wide = field[x, block]
                coupled = acc[pl.ds(pl.multiple_of(i * UNIT, SUB), UNIT), x * lanes : (x + 1) * lanes]
                grown = (wide + coupling * wide * coupled) * sea[x]
                grown = grown.astype(jnp.bfloat16).astype(jnp.float32)
                field[x, block] = grown
                values.append(grown)
            pack(0, block, values)

    def advance(e, c, source, finish):
        start, count = chunks[c]

        @pl.loop(0, count)
        def _(i):
            block = start + i
            for kind, group in ((0, plus_runs), (1, minus_runs)):
                arrived = xrecv[e, kind, block].astype(jnp.float32)
                packed[kind] = arrived
                at = 0
                for first_row, length in group:
                    halo[first_row : first_row + length, :] = packed[kind, at : at + length, :]
                    at += length
            edges = jnp.where(lane % 2 == 0, pltpu.roll(yrecv[e, 0, block], 2, 1), yrecv[e, 1, block])
            speed = column[pl.ds(pl.multiple_of(block * UNIT, SUB), UNIT), :]
            cross, along = speed * tabs_ref[0], speed * tabs_ref[1]
            results = [[] for _ in range(rows_x)]
            for t in range(tile_count):
                part = slice(t * SUB, (t + 1) * SUB)
                up_x, up_y = tabs_ref[2, part, :] > 0.5, tabs_ref[3, part, :] > 0.5
                edge = (up_y & (lane == 0)) | (jnp.logical_not(up_y) & (lane == lanes - 1))
                tiles = [source[x, block, part, :] for x in range(rows_x)]
                for x in range(rows_x):
                    j = t * rows_x + x
                    here = tiles[x]
                    lower = tiles[x - 1] if x > 0 else halo[part, :]
                    higher = tiles[x + 1] if x < rows_x - 1 else halo[part, :]
                    near_x = jnp.where(up_x, lower, higher)
                    near_y = jnp.where(up_y, pltpu.roll(here, 1, 1), pltpu.roll(here, lanes - 1, 1))
                    near_y = jnp.where(edge, pltpu.roll(edges, lanes - (2 * j + 2), 1), near_y)
                    results[x].append(
                        (here - cross[part] * (here - near_x) - along[part] * (here - near_y))
                        * sea[x][part]
                    )
            finish(block, [jnp.concatenate(r, axis=0) for r in results])

    def keep(block, values):
        for x in range(rows_x):
            first[x, block] = values[x]
        pack(1, block, values)

    def write(block, values):
        for x in range(rows_x):
            stage[pl.ds(x, UNIT, stride=rows_x), :] = values[x]
        size = rows_x * UNIT
        outv[pl.ds(pl.multiple_of(block * size, 16), size), :] = stage[0:size, :].astype(outv.dtype)

    out_copies = []
    for step in range(len(chunks) + 2):
        if step < len(chunks):
            start, count = chunks[step]
            inter_copies[step].wait()
            acc[0 : count * UNIT, :] = jnp.dot(
                inter[start * UNIT : (start + count) * UNIT, :], flat[...],
                preferred_element_type=jnp.float32,
            )
            grow(step)
            start_sends(0, step)
        if 0 <= step - 1 < len(chunks):
            wait_receives(0, step - 1)
            advance(0, step - 1, field, keep)
            start_sends(1, step - 1)
        if 0 <= step - 2:
            c = step - 2
            wait_receives(1, c)
            advance(1, c, first, write)
            start, count = chunks[c]
            part = pl.ds(start * UNIT * rows_x, count * UNIT * rows_x)
            copy = pltpu.make_async_copy(outv.at[part], out_hbm.at[part], out_sem.at[c])
            copy.start()
            out_copies.append(copy)

    for e in range(PROP):
        for c in range(len(chunks)):
            for kind in range(4):
                @pl.when(sends[kind])
                def _():
                    exchange(e, c, kind).wait_send()
    for copy in out_copies:
        copy.wait()


def shards(mesh_counts, spectrum, interaction, speeds, mask):
    comps, rows_x, lanes = spectrum.shape
    blocks = comps // UNIT
    chunks = splits(blocks)
    most = max(count for _, count in chunks)
    cosine, sine = circle()
    plus = cosine[np.arange(UNIT) % ND] > 0
    plus_runs, minus_runs = runs(plus), runs(~plus)
    half = max(int(plus.sum()), int((~plus).sum()))
    padded = -(-comps // lanes)
    speeds_rows = jnp.pad(speeds, (0, padded * lanes - comps)).reshape(padded, lanes)
    any_space = pl.BlockSpec(memory_space=pl.ANY)
    vmem = pl.BlockSpec(memory_space=pltpu.VMEM)
    f32, bf16 = jnp.float32, jnp.bfloat16
    out = pl.pallas_call(
        functools.partial(kernel, rows_x, chunks, plus_runs, minus_runs, mesh_counts),
        out_shape=jax.ShapeDtypeStruct((comps * rows_x, lanes), bf16),
        in_specs=[any_space, any_space, vmem, vmem, vmem],
        out_specs=any_space,
        scratch_shapes=[
            pltpu.VMEM((comps * rows_x, lanes), bf16),
            pltpu.VMEM((comps, comps), bf16),
            pltpu.VMEM((comps, rows_x * lanes), bf16),
            pltpu.VMEM((most * UNIT, rows_x * lanes), f32),
            pltpu.VMEM((rows_x, blocks, UNIT, lanes), f32),
            pltpu.VMEM((rows_x, blocks, UNIT, lanes), f32),
            pltpu.VMEM((padded * lanes, lanes), f32),
            pltpu.VMEM((2 * UNIT * rows_x, lanes), f32),
            pltpu.VMEM((2, half, lanes), f32),
            pltpu.VMEM((UNIT, lanes), f32),
            pltpu.VMEM((comps * rows_x, lanes), bf16),
            pltpu.VMEM((PROP, 2, blocks, half, lanes), bf16),
            pltpu.VMEM((PROP, 2, blocks, half, lanes), bf16),
            pltpu.VMEM((PROP, blocks, SUB, lanes), f32),
            pltpu.VMEM((PROP, 2, blocks, SUB, lanes), f32),
            pltpu.SemaphoreType.DMA((len(chunks) + 1,)),
            pltpu.SemaphoreType.DMA((len(chunks),)),
            pltpu.SemaphoreType.DMA((PROP, len(chunks), 4)),
            pltpu.SemaphoreType.DMA((PROP, len(chunks), 4)),
        ],
        compiler_params=pltpu.CompilerParams(
            collective_id=0, has_side_effects=True, vmem_limit_bytes=60 * 1024 * 1024
        ),
    )(
        spectrum.reshape(comps * rows_x, lanes), interaction, speeds_rows, mask,
        jnp.asarray(tables(lanes)),
    )
    return out.reshape(comps, rows_x, lanes)


def solution(mesh):
    placed = (P(None, ("member", "pts"), "sub"), P(), P(), P("pts", "sub"))
    return jax.shard_map(
        functools.partial(shards, (mesh.shape["pts"], mesh.shape["sub"])),
        mesh=mesh,
        in_specs=placed,
        out_specs=P(None, ("member", "pts"), "sub"),
        check_vma=False,
    )
```

```python
import functools
import math

import jax
import jax.numpy as jnp
import numpy as np
from jax import lax
from jax.experimental import pallas as pl
from jax.experimental.pallas import tpu as pltpu
from jax.sharding import PartitionSpec as P

ND = 36
PROP = 2
UNIT = 72
SUB = 8
CHUNKS = 4
SLOTS = 1

coupling = 0.5


def circle():
    angle = np.arange(ND, dtype=np.int32).astype(np.float32) * np.float32(2.0 * math.pi / ND)
    angle = angle.astype(np.float64)
    return np.cos(angle).astype(np.float32), np.sin(angle).astype(np.float32)


def runs(flags):
    found, start = [], None
    for i, flag in enumerate(list(flags) + [False]):
        if flag and start is None:
            start = i
        if not flag and start is not None:
            found.append((start, i - start))
            start = None
    return found


def tables(lanes):
    cosine, sine = circle()
    d = np.arange(UNIT) % ND
    rows = [np.abs(cosine[d]), np.abs(sine[d]), cosine[d] > 0, sine[d] > 0]
    return np.stack([np.broadcast_to(r.astype(np.float32)[:, None], (UNIT, lanes)) for r in rows])


def splits(blocks):
    size = max(2, blocks // CHUNKS // 2 * 2)
    starts = list(range(0, blocks, size))
    if len(starts) > 1 and blocks - starts[-1] < size:
        starts.pop()
    return [(s, (starts[i + 1] if i + 1 < len(starts) else blocks) - s) for i, s in enumerate(starts)]


def kernel(
    rows_x, chunks, plus_runs, minus_runs, counts,
    spec_hbm, inter_hbm, speeds_ref, mask_ref, tabs_ref, outv,
    specv, inter, flat, acc, field, first, column, stage, outs, packed, arrived, halo,
    xsend, xrecv, ysend, yrecv,
    load_sem, send_sem, recv_sem,
):
    lanes = flat.shape[1] // rows_x
    blocks = field.shape[1]
    tile_count = UNIT // SUB
    px, sy = lax.axis_index("pts"), lax.axis_index("sub")
    nx, ny = counts
    partner = [{"pts": px + 1}, {"pts": px - 1}, {"sub": sy + 1}, {"sub": sy - 1}]
    sends = [px < nx - 1, px > 0, sy < ny - 1, sy > 0]
    receives = [sends[1], sends[0], sends[3], sends[2]]

    spec_copy = pltpu.make_async_copy(spec_hbm, specv, load_sem.at[len(chunks)])
    spec_copy.start()
    inter_copies = []
    for c, (start, count) in enumerate(chunks):
        part = pl.ds(start * UNIT, count * UNIT)
        copy = pltpu.make_async_copy(inter_hbm.at[part], inter.at[part], load_sem.at[c])
        copy.start()
        inter_copies.append(copy)

    barrier = pltpu.get_barrier_semaphore()
    for kind in range(4):
        @pl.when(sends[kind])
        def _():
            pl.semaphore_signal(
                barrier, inc=1, device_id=partner[kind], device_id_type=pl.DeviceIdType.MESH
            )

    def exchange(e, c, kind):
        start, count = chunks[c]
        part = pl.ds(start, count)
        if kind < 2:
            source, target = xsend.at[e, kind, part], xrecv.at[e, kind, part]
        else:
            source, target = ysend.at[e, part], yrecv.at[e, kind - 2, part]
        return pltpu.make_async_remote_copy(
            src_ref=source, dst_ref=target,
            send_sem=send_sem.at[e, c, kind], recv_sem=recv_sem.at[e, c, kind],
            device_id=partner[kind], device_id_type=pl.DeviceIdType.MESH,
        )

    def start_sends(e, c):
        for kind in range(4):
            @pl.when(sends[kind])
            def _():
                exchange(e, c, kind).start()

    def wait_receives(e, c):
        for kind in range(4):
            @pl.when(receives[kind])
            def _():
                exchange(e, c, kind).wait_recv()

    for kind in range(4):
        @pl.when(jnp.logical_not(receives[kind]))
        def _():
            for e in range(PROP):
                if kind < 2:
                    xrecv[e, kind] = jnp.zeros(xrecv.shape[2:], xrecv.dtype)
                else:
                    yrecv[e, kind - 2] = jnp.zeros(yrecv.shape[2:], yrecv.dtype)

    comps = flat.shape[0]
    starts = list(range(0, comps - lanes + 1, lanes))
    if comps % lanes:
        starts.append(comps - lanes)
    for at in starts:
        row = jnp.broadcast_to(speeds_ref[0:1, at : at + lanes], (lanes, lanes))
        column[at : at + lanes, :] = row.T

    spec_copy.wait()

    def spread(block, count):
        length = count * UNIT
        whole = specv[pl.ds(pl.multiple_of(block * (rows_x * UNIT), 16), rows_x * length), :]
        stage[0 : rows_x * length, :] = whole.astype(jnp.float32)
        for x in range(rows_x):
            values = stage[pl.ds(x, length, stride=rows_x), :]
            flat[pl.ds(pl.multiple_of(block * UNIT, 16), length), x * lanes : (x + 1) * lanes] = (
                values.astype(jnp.bfloat16)
            )
            for b in range(count):
                field[x, block + b] = values[b * UNIT : (b + 1) * UNIT]

    @pl.loop(0, blocks // 2)
    def _(i):
        spread(2 * i, 2)

    if blocks % 2:
        spread(blocks - 1, 1)

    pl.semaphore_wait(barrier, sum(s.astype(jnp.int32) for s in sends))

    lane = lax.broadcasted_iota(jnp.int32, (SUB, lanes), 1)
    pair = lane // 2
    even = lane % 2 == 0
    sea = [
        jnp.broadcast_to(mask_ref[x : x + 1, :].astype(jnp.float32), (SUB, lanes))
        for x in range(rows_x)
    ]
    cosine, sine = (np.resize(v, UNIT).reshape(tile_count, SUB) for v in circle())

    def sides(t):
        found = []
        for values in (cosine[t], sine[t]):
            if np.all(values >= 0):
                found.append(True)
            elif np.all(values <= 0):
                found.append(False)
            else:
                found.append(None)
        return found

    def pack_x(e, block, slot, source):
        for kind, group, x in ((0, plus_runs, rows_x - 1), (1, minus_runs, 0)):
            at = 0
            for begin, length in group:
                packed[slot, kind, at : at + length, :] = source[x, block, begin : begin + length, :]
                at += length
            xsend[e, kind, block] = packed[slot, kind].astype(xsend.dtype)

    def grow_block(base, i, slot):
        block = base + i
        message = jnp.zeros((SUB, lanes), jnp.float32)
        for t in range(tile_count):
            part = slice(t * SUB, (t + 1) * SUB)
            place = pl.ds(pl.multiple_of(i * UNIT, SUB) + t * SUB, SUB)
            for x in range(rows_x):
                wide = field[x, block, part, :]
                coupled = acc[place, x * lanes : (x + 1) * lanes]
                grown = (wide + coupling * wide * coupled) * sea[x]
                grown = grown.astype(jnp.bfloat16).astype(jnp.float32)
                field[x, block, part, :] = grown
                j = t * rows_x + x
                message = jnp.where(pair == j, pltpu.roll(grown, 2 * j + 1, 1), message)
        ysend[0, block] = message
        pack_x(0, block, slot, field)

    def halos(e, block, slot):
        for kind, group in ((0, plus_runs), (1, minus_runs)):
            arrived[slot, kind] = xrecv[e, kind, block].astype(jnp.float32)
            at = 0
            for begin, length in group:
                halo[slot, begin : begin + length, :] = arrived[slot, kind, at : at + length, :]
                at += length

    def advance_block(e, block, slot):
        source = field if e == 0 else first
        results = []
        edges = jnp.where(even, pltpu.roll(yrecv[e, 0, block], 2, 1), yrecv[e, 1, block])
        message = jnp.zeros((SUB, lanes), jnp.float32)
        for t in range(tile_count):
            part = slice(t * SUB, (t + 1) * SUB)
            speed = column[pl.ds(pl.multiple_of(block * UNIT, SUB) + t * SUB, SUB), :]
            cross, along = speed * tabs_ref[0, part, :], speed * tabs_ref[1, part, :]
            side_x, side_y = sides(t)
            up_x = tabs_ref[2, part, :] > 0.5 if side_x is None else None
            if side_y is None:
                up_y = tabs_ref[3, part, :] > 0.5
                edge = jnp.where(up_y, lane, lanes - 1 - lane) == 0
            else:
                edge = lane == (0 if side_y else lanes - 1)
            tiles = [source[x, block, part, :] for x in range(rows_x)]
            outer = halo[slot, part, :]
            for x in range(rows_x):
                j = t * rows_x + x
                here = tiles[x]
                lower = tiles[x - 1] if x > 0 else outer
                higher = tiles[x + 1] if x < rows_x - 1 else outer
                if side_x is None:
                    near_x = jnp.where(up_x, lower, higher)
                else:
                    near_x = lower if side_x else higher
                if side_y is None:
                    near_y = jnp.where(up_y, pltpu.roll(here, 1, 1), pltpu.roll(here, lanes - 1, 1))
                else:
                    near_y = pltpu.roll(here, 1 if side_y else lanes - 1, 1)
                near_y = jnp.where(edge, pltpu.roll(edges, lanes - (2 * j + 2), 1), near_y)
                result = (here - cross * (here - near_x) - along * (here - near_y)) * sea[x]
                results.append(result)
                if e == 0:
                    message = jnp.where(pair == j, pltpu.roll(result, 2 * j + 1, 1), message)
        for t in range(tile_count):
            for x in range(rows_x):
                result = results[t * rows_x + x]
                if e == 0:
                    first[x, block, t * SUB : (t + 1) * SUB, :] = result
                else:
                    outs[slot, pl.ds(x + t * SUB * rows_x, SUB, stride=rows_x), :] = result
        if e == 0:
            ysend[1, block] = message
            pack_x(1, block, slot, first)
        else:
            size = rows_x * UNIT
            outv[pl.ds(pl.multiple_of(block * size, 16), size), :] = outs[slot].astype(outv.dtype)

    def several(count, body):
        @pl.loop(0, count // SLOTS)
        def _(i):
            body([i * SLOTS + u for u in range(SLOTS)])

        if count % SLOTS:
            body([count - count % SLOTS + u for u in range(count % SLOTS)])

    def multiply(c):
        start, count = chunks[c]
        inter_copies[c].wait()
        acc[0 : count * UNIT, :] = jnp.dot(
            inter[start * UNIT : (start + count) * UNIT, :], flat[...],
            preferred_element_type=jnp.float32,
        )

        def body(which):
            for slot, i in enumerate(which):
                grow_block(start, i, slot)

        several(count, body)
        start_sends(0, c)

    def advance(e, c):
        start, count = chunks[c]
        wait_receives(e, c)

        def body(which):
            for slot, i in enumerate(which):
                halos(e, start + i, slot)
            for slot, i in enumerate(which):
                advance_block(e, start + i, slot)

        several(count, body)
        if e == 0:
            start_sends(1, c)

    total = len(chunks)
    for c in range(total):
        multiply(c)
        if c >= 2:
            advance(0, c - 2)
    if total >= 2:
        advance(0, total - 2)
    for c in range(total - 3):
        advance(1, c)
    advance(0, total - 1)
    for c in range(max(total - 3, 0), total):
        advance(1, c)

    for e in range(PROP):
        for c in range(len(chunks)):
            for kind in range(4):
                @pl.when(sends[kind])
                def _():
                    exchange(e, c, kind).wait_send()


def flush(held, out_hbm, sem):
    copy = pltpu.make_async_copy(held, out_hbm, sem)
    copy.start()
    copy.wait()


def shards(mesh_counts, spectrum, interaction, speeds, mask):
    comps, rows_x, lanes = spectrum.shape
    blocks = comps // UNIT
    chunks = splits(blocks)
    most = max(count for _, count in chunks)
    cosine, sine = circle()
    plus = cosine[np.arange(UNIT) % ND] > 0
    plus_runs, minus_runs = runs(plus), runs(~plus)
    half = max(int(plus.sum()), int((~plus).sum()))
    any_space = pl.BlockSpec(memory_space=pltpu.HBM)
    vmem = pl.BlockSpec(memory_space=pltpu.VMEM)
    f32, bf16 = jnp.float32, jnp.bfloat16
    out = pl.pallas_call(
        functools.partial(kernel, rows_x, chunks, plus_runs, minus_runs, mesh_counts),
        out_shape=jax.ShapeDtypeStruct((comps * rows_x, lanes), bf16),
        in_specs=[any_space, any_space, vmem, vmem, vmem],
        out_specs=vmem,
        scratch_shapes=[
            pltpu.VMEM((comps * rows_x, lanes), bf16),
            pltpu.VMEM((comps, comps), bf16),
            pltpu.VMEM((comps, rows_x * lanes), bf16),
            pltpu.VMEM((most * UNIT, rows_x * lanes), f32),
            pltpu.VMEM((rows_x, blocks, UNIT, lanes), f32),
            pltpu.VMEM((rows_x, blocks, UNIT, lanes), f32),
            pltpu.VMEM((comps, lanes), f32),
            pltpu.VMEM((2 * UNIT * rows_x, lanes), f32),
            pltpu.VMEM((SLOTS, UNIT * rows_x, lanes), f32),
            pltpu.VMEM((SLOTS, 2, half, lanes), f32),
            pltpu.VMEM((SLOTS, 2, half, lanes), f32),
            pltpu.VMEM((SLOTS, UNIT, lanes), f32),
            pltpu.VMEM((PROP, 2, blocks, half, lanes), bf16),
            pltpu.VMEM((PROP, 2, blocks, half, lanes), bf16),
            pltpu.VMEM((PROP, blocks, SUB, lanes), f32),
            pltpu.VMEM((PROP, 2, blocks, SUB, lanes), f32),
            pltpu.SemaphoreType.DMA((len(chunks) + 1,)),
            pltpu.SemaphoreType.DMA((PROP, len(chunks), 4)),
            pltpu.SemaphoreType.DMA((PROP, len(chunks), 4)),
        ],
        compiler_params=pltpu.CompilerParams(
            collective_id=0, has_side_effects=True, vmem_limit_bytes=62 * 1024 * 1024
        ),
    )(
        spectrum.reshape(comps * rows_x, lanes), interaction, speeds.reshape(1, comps), mask,
        jnp.asarray(tables(lanes)),
    )
    out = pl.pallas_call(
        flush,
        out_shape=jax.ShapeDtypeStruct((comps * rows_x, lanes), bf16),
        in_specs=[vmem],
        out_specs=any_space,
        scratch_shapes=[pltpu.SemaphoreType.DMA],
        compiler_params=pltpu.CompilerParams(vmem_limit_bytes=8 * 1024 * 1024),
    )(out)
    return out.reshape(comps, rows_x, lanes)


def solution(mesh):
    placed = (P(None, ("member", "pts"), "sub"), P(), P(), P("pts", "sub"))
    return jax.shard_map(
        functools.partial(shards, (mesh.shape["pts"], mesh.shape["sub"])),
        mesh=mesh,
        in_specs=placed,
        out_specs=P(None, ("member", "pts"), "sub"),
        check_vma=False,
    )
```
